128 devices in a mesh: dp: 16 (over x, z), mp: 8 (over y, core).
Axes of the slice: x: 4, y: 4, z: 4, core: 2. Of those that a mesh axis runs over, the one named last changes fastest.
Arguments:
- hidden_in: bfloat16 [2, 2048, 3584], P(None, 'dp', 'mp'), may hold values from -6 to 6
- out_grad: bfloat16 [2, 2048, 3584], P(None, 'dp', 'mp'), may hold values from -3072 to 3072
- pack_fill: int32 [2, 16], P(None, 'dp'), may hold values from 1 to 128, as said below
- norm_gain: float32 [3584], P('mp'), may hold values from 0.5 to 1.5
- up_weight: bfloat16 [3584, 7168], P(None, 'mp'), may hold values from -0.09375 to 0.09375
- down_weight: bfloat16 [7168, 3584], P('mp'), may hold values from -0.0625 to 0.0625
Outputs:
- in_grad: bfloat16 [2, 2048, 3584], P(None, 'dp', 'mp')
- up_grad: float32 [3584, 7168], P('dp', 'mp')
- down_grad: float32 [7168, 3584], P('mp', 'dp')
- gain_grad: float32 [3584], P('mp')
The draws below stay inside these ranges and needn't reach their ends.
Inputs may be any that keep to these rules, and one draw needn't show every extreme that they name: pack_fill[m, p] real tokens stand at the start of pack p of microbatch m (positions p * 128 onward); the other positions of the pack are padding and carry no loss. In every draw the last pack of the first microbatch is full.
All inputs are finite; a program needn't handle non-finite values.
Results may differ from the reference program's by a relative error of at most 0.014.
Values may be sent and summed in bfloat16 or wider, within the bound.
No kernel may reach another device: no remote copies, remote signals or barrier semaphores. Data moves between devices by JAX's collectives and lax.ppermute only.
A program may use at most 128 MiB of HBM per device.

```python
import jax
import jax.numpy as jnp
from jax import lax

D = 3584
FFW = 7168
TOK_DEV = 128
MICRO = 2
TOKENS = 2048
N_MP = 8


def draw_pack_fill(key, part):
    pack_count = TOKENS // TOK_DEV
    pack_pos = jnp.arange(pack_count, dtype=jnp.int32)
    fill_top = TOK_DEV // 16 + 15 * TOK_DEV // 16 * pack_pos * pack_pos // ((pack_count - 1) * (pack_count - 1))
    fill_low = fill_top // 2 + 1
    drawn = jax.random.randint(key, (MICRO, pack_count), fill_low[None, :], fill_top[None, :] + 1, dtype=jnp.int32)
    return drawn.at[0, pack_count - 1].set(TOK_DEV)


def block_scale(stream_key, shape, split, low, top_value):
    def one(dim, shards_of):
        heights = jax.random.uniform(jax.random.fold_in(jax.random.fold_in(stream_key, 6), dim), (shards_of,), jnp.float32, low / len(split), top_value / len(split))
        return jnp.repeat(jnp.exp(heights), shape[dim] // shards_of).reshape((-1,) + (1,) * (len(shape) - dim - 1))

    gain = one(*split[0])
    for cut in split[1:]:
        gain = gain * one(*cut)
    return gain


def normal_values(rng, shape, deviation, most, split=(), kind=jnp.bfloat16):
    loudness = block_scale(rng, shape, split, -0.22, 0.18) if split else 1.0
    entries = jax.random.normal(rng, shape, jnp.float32) * deviation * loudness
    return jnp.minimum(jnp.maximum(entries, -most), most).astype(kind)


def setup_inputs(seed: int = 0) -> dict:
    keys = jax.random.split(jax.random.key(seed), 7)
    hidden_in = normal_values(keys[0], (MICRO, TOKENS, D), 1.0, 6.0, ((1, 16), (2, 8)))
    out_grad = normal_values(keys[1], (MICRO, TOKENS, D), (MICRO * TOKENS // 8), 3072.0, ((1, 16), (2, 8)))
    pack_fill = draw_pack_fill(jax.random.fold_in(keys[6], 71), 0)
    norm_gain = jnp.clip(1.0 + 0.1 * jax.random.normal(keys[3], (D,), jnp.float32), 0.5, 1.5)
    up_weight = normal_values(keys[4], (D, FFW), D ** -0.5, 0.09375, ((1, 8),))
    down_weight = normal_values(keys[5], (FFW, D), FFW ** -0.5, 0.0625, ((0, 8),))
    return {"hidden_in": hidden_in, "out_grad": out_grad, "pack_fill": pack_fill, "norm_gain": norm_gain, "up_weight": up_weight, "down_weight": down_weight}


epsilon = 1e-06

def gelu_tanh(value):
    return jax.nn.gelu(value, approximate=True)

def contract_rows(left, right):
    return lax.dot_general(left, right, (((0,), (0,)), ((), ())), preferred_element_type=jnp.float32)

def contract_cols(left, right):
    return lax.dot_general(left, right, (((1,), (1,)), ((), ())), preferred_element_type=jnp.float32)

def group_sums(grad_pre, up_weight):
    row_count = grad_pre.shape[0]
    model_width = up_weight.shape[0]
    group_width = up_weight.shape[1] // N_MP
    pre_groups = grad_pre.reshape(row_count, N_MP, group_width).transpose(1, 0, 2)
    weight_groups = up_weight.reshape(model_width, N_MP, group_width).transpose(1, 0, 2)

    def add_group(total, pair):
        rounded = contract_cols(pair[0], pair[1]).astype(jnp.bfloat16)
        rounded = lax.optimization_barrier(rounded)
        return (total + rounded.astype(jnp.float32), None)
    total, unused = lax.scan(add_group, jnp.zeros((row_count, model_width), jnp.float32), (pre_groups, weight_groups))
    return total

def micro_grads(hidden_rows, grad_rows, live_mask, inv_count, norm_gain, up_weight, down_weight):
    model_width = hidden_rows.shape[1]
    values = hidden_rows.astype(jnp.float32)
    inv_rms = lax.rsqrt(lax.optimization_barrier(jnp.sum(values * values, axis=1, keepdims=True)) / model_width + epsilon)
    normed = (values * inv_rms * norm_gain[None, :]).astype(jnp.bfloat16)
    pre_act = jnp.dot(normed, up_weight, preferred_element_type=jnp.float32)
    activated = gelu_tanh(pre_act).astype(jnp.bfloat16)
    scaled = (grad_rows.astype(jnp.float32) * live_mask[:, None] * inv_count).astype(jnp.bfloat16)
    grad_act = contract_cols(scaled, down_weight)
    grad_pre = jax.vjp(gelu_tanh, pre_act)[1](grad_act)[0].astype(jnp.bfloat16)
    grad_normed = group_sums(grad_pre, up_weight)
    row_dot = lax.optimization_barrier(jnp.sum(grad_normed * norm_gain[None, :] * values, axis=1, keepdims=True))
    cubed = inv_rms * inv_rms * inv_rms
    in_rows = scaled.astype(jnp.float32) + norm_gain[None, :] * grad_normed * inv_rms - values * cubed * row_dot / model_width
    gain_term = lax.optimization_barrier(jnp.sum(grad_normed * values * inv_rms, axis=0))
    return (in_rows.astype(jnp.bfloat16), contract_rows(normed, grad_pre), contract_rows(activated, scaled), gain_term)

def reference(hidden_in, out_grad, pack_fill, norm_gain, up_weight, down_weight):
    token_total = jnp.sum(pack_fill).astype(jnp.float32)
    inv_count = 1.0 / token_total
    position = jnp.arange(TOKENS, dtype=jnp.int32)
    pack_index = position // TOK_DEV
    offset = position % TOK_DEV
    up_grad = jnp.zeros(up_weight.shape, jnp.float32)
    down_grad = jnp.zeros(down_weight.shape, jnp.float32)
    gain_grad = jnp.zeros(norm_gain.shape, jnp.float32)
    in_parts = []
    for micro_index in range(MICRO):
        live_mask = (offset < pack_fill[micro_index][pack_index]).astype(jnp.float32)
        in_rows, up_term, down_term, gain_term = micro_grads(hidden_in[micro_index], out_grad[micro_index], live_mask, inv_count, norm_gain, up_weight, down_weight)
        up_grad = up_grad + up_term
        down_grad = down_grad + down_term
        gain_grad = gain_grad + gain_term
        in_parts.append(in_rows)
    return (jnp.stack(in_parts), up_grad, down_grad, gain_grad)
```

```python
import jax
import jax.numpy as jnp
from jax import lax
from jax.experimental import pallas as pl
from jax.experimental.pallas import tpu as pltpu
from jax.sharding import Mesh
from jax.sharding import PartitionSpec as P

INTERPRET = False
EPS = 1e-06
EXTRA = 16
GELU_A = 0.7978845608028654
GELU_B = 0.044715

F32 = jnp.float32
BF16 = jnp.bfloat16


def moved(value, axis, step):
    size = lax.axis_size(axis)
    return lax.ppermute(value, axis, [(i, (i + step) % size) for i in range(size)])


def ring_of(value, axis):
    return tuple(moved(value, axis, step) for step in (1, 2, 3))


def total_over(value, axes):
    for axis in axes:
        a, b, c = ring_of(value, axis)
        value = (value + b) + (a + c)
    return value


def spec(space=pltpu.VMEM):
    return pl.BlockSpec(memory_space=space)


def call(body, outs, ins, scratch=(), flops=0, moved_bytes=0, name="local"):
    return pl.pallas_call(
        body,
        out_shape=[jax.ShapeDtypeStruct(s, d) for s, d in outs],
        in_specs=[spec(space) for _, space in ins],
        out_specs=[spec() for _ in outs],
        scratch_shapes=list(scratch),
        cost_estimate=pl.CostEstimate(flops=flops, bytes_accessed=moved_bytes, transcendentals=0),
        compiler_params=pltpu.CompilerParams(vmem_limit_bytes=48 * 1024 * 1024),
        interpret=INTERPRET,
        name=name,
    )(*[a for a, _ in ins])


V, S, H = pltpu.VMEM, pltpu.SMEM, pl.ANY


def split3(value):
    hi = value.astype(BF16)
    rest = value - hi.astype(F32)
    mid = rest.astype(BF16)
    return hi, mid, (rest - mid.astype(F32)).astype(BF16)


def extra_rows(value):
    parts = [p.astype(F32) for p in split3(value)]
    row = lax.broadcasted_iota(jnp.int32, (EXTRA, value.shape[-1]), 0)
    out = jnp.where(row == 0, parts[0], 0.0)
    out = jnp.where(row == 1, parts[1], out)
    return jnp.where(row == 2, parts[2], out).astype(BF16)


def sum_extra(rows):
    return jnp.sum(rows.astype(F32), axis=0, keepdims=True)


def dot(left, right, dims):
    return lax.dot_general(left, right, (dims, ((), ())), preferred_element_type=F32)


def live_row(sc, tok):
    pos = lax.broadcasted_iota(jnp.int32, (1, 2 * tok), 1)
    in_first = pos < tok
    limit = jnp.where(in_first, sc[4], sc[5] + tok)
    return (pos < limit).astype(F32)


def prepare(hidden_t, gain_mat):
    micro, width, tok = hidden_t.shape

    def body(h_ref, g_ref, out_ref):
        for m in range(micro):
            h = h_ref[m].astype(F32)
            out_ref[m, :width, :] = (h * g_ref[...]).astype(BF16)
            out_ref[m, width:, :] = extra_rows(jnp.sum(h * h, axis=0, keepdims=True))

    return call(body, [((micro, width + EXTRA, tok), BF16)], [(hidden_t, V), (gain_mat, V)], name="prepare")[0]


def forward_part(sc, up, own, other):
    micro, padded, tok = own[0].shape
    width = padded - EXTRA
    ff = up.shape[1]
    d = up.shape[0]
    pair = 2 * width
    cols = micro * tok

    def body(sc, up_ref, *refs):
        r, s = refs[0:4], refs[4:8]
        act_ref, pre_ref, inv_ref, hown_ref, h1, h2, h3, wbuf, hbuf, sem = refs[8:]
        x, y, c = sc[0], sc[1], sc[3]

        def fetch(k):
            start = pl.multiple_of(((y + 4 - k) % 4) * pair, pair)
            return pltpu.make_async_copy(up_ref.at[pl.ds(start, pair), :], wbuf.at[k], sem.at[k])

        for k in range(4):
            fetch(k).start()
        mine = pl.multiple_of(c * width, width)
        its = pl.multiple_of((1 - c) * width, width)
        squares = []
        for m in range(micro):
            total = jnp.zeros((1, tok), F32)
            for k in range(4):
                hbuf[k, pl.ds(mine, width), m * tok : (m + 1) * tok] = r[k][m, :width, :]
                hbuf[k, pl.ds(its, width), m * tok : (m + 1) * tok] = s[k][m, :width, :]
                total = total + sum_extra(r[k][m, width:, :]) + sum_extra(s[k][m, width:, :])
            squares.append(total)
        inv = lax.rsqrt(jnp.concatenate(squares, axis=1) / d + EPS)
        inv_ref[...] = jnp.broadcast_to(inv, inv_ref.shape)
        hown_ref[...] = hbuf[(y - x + 4) % 4]
        for k, ref in ((1, h1), (2, h2), (3, h3)):
            ref[...] = hbuf[(y - x - k + 8) % 4, pl.ds(mine, width), :]
        acc = None
        for k in range(4):
            fetch(k).wait()
            part = dot(hbuf[k].T, wbuf[k], ((1,), (0,)))
            acc = part if acc is None else acc + part
        pre = acc.T * inv
        pre_ref[...] = pre
        act = 0.5 * pre * (1.0 + jnp.tanh(GELU_A * (pre + GELU_B * pre * pre * pre)))
        act_ref[...] = (act * live_row(sc, tok)).astype(BF16)

    return call(
        body,
        [
            ((ff, cols), BF16),
            ((ff, cols), F32),
            ((8, cols), F32),
            ((pair, cols), BF16),
        ]
        + [((width, cols), BF16)] * 3,
        [(sc, S), (up, H)] + [(a, V) for a in (*own, *other)],
        [
            pltpu.VMEM((4, pair, ff), BF16),
            pltpu.VMEM((4, pair, cols), BF16),
            pltpu.SemaphoreType.DMA((4,)),
        ],
        flops=2 * d * ff * cols,
        moved_bytes=d * ff * 2,
        name="forward_part",
    )


def backward_part(sc, down, own, other, pre, inv):
    micro, width, tok = own[0].shape
    ff = down.shape[0]
    d = down.shape[1]
    pair = 2 * width
    quarter = pair // 4
    cols = micro * tok

    def body(sc, down_ref, *refs):
        r, s = refs[0:4], refs[4:8]
        pre_ref, inv_ref, gp_ref, rd_ref, oown_ref, o1, o2, o3, wbuf, obuf, sem = refs[8:]
        y, z, c = sc[1], sc[2], sc[3]

        def fetch(k):
            start = pl.multiple_of(((y + 4 - k) % 4) * pair, pair)
            return pltpu.make_async_copy(down_ref.at[:, pl.ds(start, pair)], wbuf.at[k], sem.at[k])

        for k in range(4):
            fetch(k).start()
        mine = pl.multiple_of(c * width, width)
        its = pl.multiple_of((1 - c) * width, width)
        for m in range(micro):
            for k in range(4):
                obuf[k, pl.ds(mine, width), m * tok : (m + 1) * tok] = r[k][m]
                obuf[k, pl.ds(its, width), m * tok : (m + 1) * tok] = s[k][m]
        for k, ref in ((0, oown_ref), (1, o1), (2, o2), (3, o3)):
            row = pl.multiple_of(((z + k) % 4) * quarter, quarter)
            for j in range(4):
                block = obuf[j, pl.ds(row, quarter), :]
                ref[j] = block if k == 0 else jnp.where(c == 0, block[:, :tok], block[:, tok:])
        acc = None
        for k in range(4):
            fetch(k).wait()
            part = dot(wbuf[k], obuf[k], ((1,), (0,)))
            acc = part if acc is None else acc + part
        pre = pre_ref[...]
        cube = GELU_B * pre * pre
        t = jnp.tanh(GELU_A * (pre + cube * pre))
        slope = 0.5 * (1.0 + t) + 0.5 * pre * (1.0 - t * t) * (GELU_A * (1.0 + 3.0 * cube))
        gp = (acc * slope * (inv_ref[0:1, :] * live_row(sc, tok))).astype(BF16)
        gp_ref[...] = gp
        rd = jnp.sum(gp.astype(F32) * pre, axis=0, keepdims=True)
        rd_ref[...] = jnp.broadcast_to(rd, rd_ref.shape)

    return call(
        body,
        [
            ((ff, cols), BF16),
            ((8, cols), F32),
            ((4, quarter, cols), BF16),
        ]
        + [((4, quarter, tok), BF16)] * 3,
        [(sc, S), (down, H)] + [(a, V) for a in (*own, *other)] + [(pre, V), (inv, V)],
        [
            pltpu.VMEM((4, ff, pair), BF16),
            pltpu.VMEM((4, pair, cols), BF16),
            pltpu.SemaphoreType.DMA((4,)),
        ],
        flops=2 * d * ff * cols,
        moved_bytes=d * ff * 2,
        name="backward_part",
    )


def normed_part(sc, up, gp, rd):
    d, ff = up.shape
    pair = d // 4
    width = pair // 2
    cols = gp.shape[1]

    def body(sc, up_ref, gp_ref, rd_ref, pown_ref, psib_ref, wbuf, sem):
        y, c = sc[1], sc[3]

        def fetch(k):
            start = pl.multiple_of(((y + k) % 4) * pair, pair)
            return pltpu.make_async_copy(up_ref.at[pl.ds(start, pair), :], wbuf.at[k], sem.at[k])

        for k in range(4):
            fetch(k).start()
        mine = pl.multiple_of(c * width, width)
        its = pl.multiple_of((1 - c) * width, width)
        gp = gp_ref[...]
        for k in range(4):
            fetch(k).wait()
            psib_ref[k, :width, :] = dot(wbuf[k, pl.ds(its, width), :], gp, ((1,), (0,))).astype(BF16)
            pown_ref[k] = dot(wbuf[k, pl.ds(mine, width), :], gp, ((1,), (0,)))
            psib_ref[k, width:, :] = extra_rows(rd_ref[0:1, :])

    return call(
        body,
        [((4, width, cols), F32), ((4, width + EXTRA, cols), BF16)],
        [(sc, S), (up, H), (gp, V), (rd, V)],
        [pltpu.VMEM((4, pair, ff), BF16), pltpu.SemaphoreType.DMA((4,))],
        flops=2 * d * ff * cols,
        moved_bytes=d * ff * 2,
        name="normed_part",
    )


def pair_sum(pown, psib, rd):
    width, cols = pown.shape[1:]

    def body(p_ref, s_ref, rd_ref, q0, rd0, q1, q2, q3):
        total = rd_ref[0:1, :] + sum_extra(s_ref[0, width:, :])
        q0[...] = p_ref[0] + s_ref[0, :width, :].astype(F32)
        rd0[...] = jnp.broadcast_to(total, rd0.shape)
        tail = extra_rows(total)
        for k, ref in ((1, q1), (2, q2), (3, q3)):
            ref[:width, :] = (p_ref[k] + s_ref[k, :width, :].astype(F32)).astype(BF16)
            ref[width:, :] = tail

    return call(
        body,
        [((width, cols), F32), ((8, cols), F32)] + [((width + EXTRA, cols), BF16)] * 3,
        [(pown, V), (psib, V), (rd, V)],
        name="pair_sum",
    )


def input_grad(sc, q0, rd0, recv, hidden_t, out_t, gain_mat, inv, inv_count):
    micro, width, tok = hidden_t.shape

    def body(sc, q0, rd0, r1, r2, r3, h_ref, o_ref, g_ref, inv_ref, ic_ref, out_ref, gain_ref):
        d = 8 * width
        grad = q0[...]
        rd = rd0[0:1, :]
        for ref in (r1, r2, r3):
            grad = grad + ref[:width, :].astype(F32)
            rd = rd + sum_extra(ref[width:, :])
        live = live_row(sc, tok)
        ic = ic_ref[0:1, :]
        factor = inv_ref[0:1, :] * rd / d
        gain = jnp.zeros((width, tok), F32)
        for m in range(micro):
            cut = slice(m * tok, (m + 1) * tok)
            h = h_ref[m].astype(F32)
            scaled = (o_ref[m].astype(F32) * (live[:, cut] * ic)).astype(BF16).astype(F32)
            rest = g_ref[...] * grad[:, cut] - h * factor[:, cut]
            out_ref[m] = (scaled + rest * ic).astype(BF16)
            gain = gain + grad[:, cut] * h
        gain_ref[...] = jnp.sum(gain, axis=1, keepdims=True) * ic[:, :1]

    return call(
        body,
        [((micro, width, tok), BF16), ((width, 1), F32)],
        [(sc, S)] + [(a, V) for a in (q0, rd0, *recv, hidden_t, out_t, gain_mat, inv, inv_count)],
        name="input_grad",
    )


def up_part(sc, hown, mine, its, gps):
    pair, cols = hown.shape
    width = pair // 2
    ff = gps[0].shape[0]
    rows = pair // 4

    def body(sc, hown_ref, m1, m2, m3, i1, i2, i3, g0, g1, g2, g3, b0, b1, b2, b3, hbuf, gbuf, acc):
        z, c = sc[2], sc[3]
        lo = pl.multiple_of(c * width, width)
        hi = pl.multiple_of((1 - c) * width, width)
        hbuf[:, :cols] = hown_ref[...]
        for k, (a, b) in enumerate(((m1, i1), (m2, i2), (m3, i3)), 1):
            hbuf[pl.ds(lo, width), k * cols : (k + 1) * cols] = a[...]
            hbuf[pl.ds(hi, width), k * cols : (k + 1) * cols] = b[...]
        for k, g in enumerate((g0, g1, g2, g3)):
            gbuf[:, k * cols : (k + 1) * cols] = g[...]
        acc[...] = dot(hbuf[...], gbuf[...], ((1,), (1,)))
        for k, ref in enumerate((b0, b1, b2, b3)):
            start = pl.multiple_of(((z + k) % 4) * rows, rows)
            ref[...] = acc[pl.ds(start, rows), :].astype(ref.dtype)

    return call(
        body,
        [((rows, ff), F32)] + [((rows, ff), BF16)] * 3,
        [(sc, S)] + [(a, V) for a in (hown, *mine, *its, *gps)],
        [
            pltpu.VMEM((pair, 4 * cols), BF16),
            pltpu.VMEM((ff, 4 * cols), BF16),
            pltpu.VMEM((pair, ff), F32),
        ],
        flops=2 * pair * ff * cols * 4,
        name="up_part",
    )


def down_part(sc, oown, mine, its, acts):
    _, rows, cols = oown.shape
    tok = cols // 2
    ff = acts[0].shape[0]
    pair = 4 * rows

    def body(sc, oown_ref, m1, m2, m3, i1, i2, i3, a0, a1, a2, a3, b0, b1, b2, b3, obuf, abuf, acc):
        x, y, c = sc[0], sc[1], sc[3]
        for j in range(4):
            cut = slice(j * rows, (j + 1) * rows)
            obuf[cut, :cols] = oown_ref[j]
            for k, (a, b) in enumerate(((m1, i1), (m2, i2), (m3, i3)), 1):
                left, right = a[j], b[j]
                obuf[cut, k * cols : k * cols + tok] = jnp.where(c == 0, left, right)
                obuf[cut, k * cols + tok : (k + 1) * cols] = jnp.where(c == 0, right, left)
        for k, a in enumerate((a0, a1, a2, a3)):
            abuf[:, k * cols : (k + 1) * cols] = a[...]
        acc[...] = dot(obuf[...], abuf[...], ((1,), (1,)))
        for k, ref in enumerate((b0, b1, b2, b3)):
            start = pl.multiple_of(((y - x - k + 8) % 4) * rows, rows)
            ref[...] = acc[pl.ds(start, rows), :].astype(ref.dtype)

    return call(
        body,
        [((rows, ff), F32)] + [((rows, ff), BF16)] * 3,
        [(sc, S)] + [(a, V) for a in (oown, *mine, *its, *acts)],
        [
            pltpu.VMEM((pair, 4 * cols), BF16),
            pltpu.VMEM((ff, 4 * cols), BF16),
            pltpu.VMEM((pair, ff), F32),
        ],
        flops=2 * pair * ff * cols * 4,
        name="down_part",
    )


def at_owner(blocks, axis):
    return (blocks[0],) + tuple(moved(blocks[k], axis, k) for k in (1, 2, 3))


def add_up(blocks, inv_count):
    first, *rest = blocks

    def body(own, r1, r2, r3, ic_ref, out_ref):
        total = own[...] + r1[...].astype(F32) + (r2[...].astype(F32) + r3[...].astype(F32))
        out_ref[...] = total * ic_ref[0:1, 0:1]

    return call(body, [(first.shape, F32)], [(a, V) for a in (first, *rest, inv_count)], name="add_up")[0]


def on_device(hidden_in, out_grad, pack_fill, norm_gain, up_weight, down_weight):
    hidden_t = jnp.swapaxes(hidden_in, 1, 2)
    out_t = jnp.swapaxes(out_grad, 1, 2)
    _, width, tok = hidden_t.shape
    fills = pack_fill[:, 0]
    place = [lax.axis_index(a) for a in ("x", "y", "z", "c")]
    sc = jnp.concatenate([jnp.stack(place).astype(jnp.int32), fills, jnp.zeros((2,), jnp.int32)])
    gain_mat = jnp.broadcast_to(norm_gain[:, None], (width, tok))

    payload = prepare(hidden_t, gain_mat)
    h_own = (payload,) + ring_of(payload, "y")
    h_other = tuple(moved(a, "c", 1) for a in h_own)
    o_own = (out_t,) + ring_of(out_t, "y")
    o_other = tuple(moved(a, "c", 1) for a in o_own)

    count = jnp.broadcast_to(jnp.sum(fills).astype(F32), (8, 128))
    inv_count = 1.0 / total_over(count, ("x", "z"))

    act, pre, inv, h_home, *h_send = forward_part(sc, up_weight, h_own, h_other)
    acts = (act,) + ring_of(act, "z")
    h_mine = tuple(moved(a, "x", k) for k, a in enumerate(h_send, 1))
    h_its = tuple(moved(a, "c", 1) for a in h_mine)

    gp, rd, o_home, *o_send = backward_part(sc, down_weight, o_own, o_other, pre, inv)
    gps = (gp,) + ring_of(gp, "x")
    o_mine = tuple(moved(a, "z", k) for k, a in enumerate(o_send, 1))
    o_its = tuple(moved(a, "c", 1) for a in o_mine)

    pown, psib = normed_part(sc, up_weight, gp, rd)
    q0, rd0, *q_send = pair_sum(pown, moved(psib, "c", 1), rd)
    q_recv = tuple(moved(a, "y", k) for k, a in enumerate(q_send, 1))
    in_t, gain = input_grad(sc, q0, rd0, q_recv, hidden_t, out_t, gain_mat, inv, inv_count)
    gain_grad = total_over(gain[:, 0], ("x", "z"))

    down_blocks = at_owner(down_part(sc, o_home, o_mine, o_its, acts), "x")
    up_blocks = at_owner(up_part(sc, h_home, h_mine, h_its, gps), "z")
    down_grad = add_up(down_blocks, inv_count).T
    up_grad = add_up(up_blocks, inv_count)
    return (jnp.swapaxes(in_t, 1, 2), up_grad, down_grad, gain_grad)


def solution(mesh):
    split = Mesh(mesh.devices.reshape(4, 4, 4, 2), ("x", "z", "y", "c"))
    dp, mp = ("x", "z"), ("y", "c")
    in_specs = (
        P(None, dp, mp),
        P(None, dp, mp),
        P(None, dp),
        P(mp),
        P(None, mp),
        P(mp, None),
    )
    out_specs = (P(None, dp, mp), P(dp, mp), P(mp, dp), P(mp))
    return jax.shard_map(
        on_device, mesh=split, in_specs=in_specs, out_specs=out_specs, check_vma=False
    )
```

```python
import jax
import jax.numpy as jnp
from jax import lax
from jax.experimental import pallas as pl
from jax.experimental.pallas import tpu as pltpu
from jax.sharding import Mesh
from jax.sharding import PartitionSpec as P

INTERPRET = False
MIB = 1024 * 1024
EPS = 1e-06
EXTRA = 16
GELU_A = 0.7978845608028654
GELU_B = 0.044715

F32 = jnp.float32
BF16 = jnp.bfloat16


def moved(value, axis, step):
    size = lax.axis_size(axis)
    return lax.ppermute(value, axis, [(i, (i + step) % size) for i in range(size)])


def ring_of(value, axis):
    return tuple(moved(value, axis, step) for step in (1, 2, 3))


def total_over(value, axes):
    for axis in axes:
        a, b, c = ring_of(value, axis)
        value = (value + b) + (a + c)
    return value


def spec(space=pltpu.VMEM):
    return pl.BlockSpec(memory_space=space)


def call(body, outs, ins, scratch=(), flops=0, moved_bytes=0, limit=8):
    return pl.pallas_call(
        body,
        out_shape=[jax.ShapeDtypeStruct(s, d) for s, d in outs],
        in_specs=[spec(space) for _, space in ins],
        out_specs=[spec() for _ in outs],
        scratch_shapes=list(scratch),
        cost_estimate=pl.CostEstimate(flops=flops, bytes_accessed=moved_bytes, transcendentals=0),
        compiler_params=pltpu.CompilerParams(vmem_limit_bytes=limit * MIB),
        interpret=INTERPRET,
    )(*[a for a, _ in ins])


V, S, H = pltpu.VMEM, pltpu.SMEM, pltpu.HBM


def split3(value):
    hi = value.astype(BF16)
    rest = value - hi.astype(F32)
    mid = rest.astype(BF16)
    return hi, mid, (rest - mid.astype(F32)).astype(BF16)


def extra_rows(value):
    parts = [p.astype(F32) for p in split3(value)]
    row = lax.broadcasted_iota(jnp.int32, (EXTRA, value.shape[-1]), 0)
    out = jnp.where(row == 0, parts[0], 0.0)
    out = jnp.where(row == 1, parts[1], out)
    return jnp.where(row == 2, parts[2], out).astype(BF16)


def sum_extra(rows):
    return jnp.sum(rows.astype(F32), axis=0, keepdims=True)


def dot(left, right, dims):
    return lax.dot_general(left, right, (dims, ((), ())), preferred_element_type=F32)


def live_row(sc, tok):
    pos = lax.broadcasted_iota(jnp.int32, (1, 2 * tok), 1)
    in_first = pos < tok
    limit = jnp.where(in_first, sc[4], sc[5] + tok)
    return (pos < limit).astype(F32)


def prepare(hidden_t, gain_mat):
    micro, width, tok = hidden_t.shape

    def body(h_ref, g_ref, out_ref):
        for m in range(micro):
            h = h_ref[m].astype(F32)
            out_ref[m, :width, :] = (h * g_ref[...]).astype(BF16)
            out_ref[m, width:, :] = extra_rows(jnp.sum(h * h, axis=0, keepdims=True))

    return call(body, [((micro, width + EXTRA, tok), BF16)], [(hidden_t, V), (gain_mat, V)])[0]


def forward_part(sc, up, own, other):
    micro, padded, tok = own[0].shape
    width = padded - EXTRA
    ff = up.shape[1]
    d = up.shape[0]
    pair = 2 * width
    cols = micro * tok

    def body(sc, up_ref, *refs):
        r, s = refs[0:4], refs[4:8]
        act_ref, pre_ref, inv_ref, hown_ref, h1, h2, h3, wbuf, hbuf, sem = refs[8:]
        x, y, c = sc[0], sc[1], sc[3]

        def fetch(k):
            start = pl.multiple_of(((y + 4 - k) % 4) * pair, pair)
            return pltpu.make_async_copy(up_ref.at[pl.ds(start, pair), :], wbuf.at[k], sem.at[k])

        for k in range(4):
            fetch(k).start()
        mine = pl.multiple_of(c * width, width)
        its = pl.multiple_of((1 - c) * width, width)
        squares = []
        for m in range(micro):
            total = jnp.zeros((1, tok), F32)
            for k in range(4):
                hbuf[k, pl.ds(mine, width), m * tok : (m + 1) * tok] = r[k][m, :width, :]
                hbuf[k, pl.ds(its, width), m * tok : (m + 1) * tok] = s[k][m, :width, :]
                total = total + sum_extra(r[k][m, width:, :]) + sum_extra(s[k][m, width:, :])
            squares.append(total)
        inv = lax.rsqrt(jnp.concatenate(squares, axis=1) / d + EPS)
        inv_ref[...] = jnp.broadcast_to(inv, inv_ref.shape)
        hown_ref[...] = hbuf[(y - x + 4) % 4]
        for k, ref in ((1, h1), (2, h2), (3, h3)):
            ref[...] = hbuf[(y - x - k + 8) % 4, pl.ds(mine, width), :]
        acc = None
        for k in range(4):
            fetch(k).wait()
            part = dot(hbuf[k].T, wbuf[k], ((1,), (0,)))
            acc = part if acc is None else acc + part
        pre = acc.T * inv
        pre_ref[...] = pre
        act = 0.5 * pre * (1.0 + jnp.tanh(GELU_A * (pre + GELU_B * pre * pre * pre)))
        act_ref[...] = (act * live_row(sc, tok)).astype(BF16)

    return call(
        body,
        [
            ((ff, cols), BF16),
            ((ff, cols), F32),
            ((8, cols), F32),
            ((pair, cols), BF16),
        ]
        + [((width, cols), BF16)] * 3,
        [(sc, S), (up, H)] + [(a, V) for a in (*own, *other)],
        [
            pltpu.VMEM((4, pair, ff), BF16),
            pltpu.VMEM((4, pair, cols), BF16),
            pltpu.SemaphoreType.DMA((4,)),
        ],
        flops=2 * d * ff * cols,
        moved_bytes=d * ff * 2,
        limit=20,
    )


def backward_part(sc, down, own, other, pre, inv):
    micro, width, tok = own[0].shape
    ff = down.shape[0]
    d = down.shape[1]
    pair = 2 * width
    quarter = pair // 4
    cols = micro * tok

    def body(sc, down_ref, *refs):
        r, s = refs[0:4], refs[4:8]
        pre_ref, inv_ref, gp_ref, rd_ref, oown_ref, o1, o2, o3, wbuf, obuf, sem = refs[8:]
        y, z, c = sc[1], sc[2], sc[3]

        def fetch(k):
            start = pl.multiple_of(((y + 4 - k) % 4) * pair, pair)
            return pltpu.make_async_copy(down_ref.at[:, pl.ds(start, pair)], wbuf.at[k], sem.at[k])

        for k in range(4):
            fetch(k).start()
        mine = pl.multiple_of(c * width, width)
        its = pl.multiple_of((1 - c) * width, width)
        for m in range(micro):
            for k in range(4):
                obuf[k, pl.ds(mine, width), m * tok : (m + 1) * tok] = r[k][m]
                obuf[k, pl.ds(its, width), m * tok : (m + 1) * tok] = s[k][m]
        for k, ref in ((0, oown_ref), (1, o1), (2, o2), (3, o3)):
            row = pl.multiple_of(((z + k) % 4) * quarter, quarter)
            for j in range(4):
                block = obuf[j, pl.ds(row, quarter), :]
                ref[j] = block if k == 0 else jnp.where(c == 0, block[:, :tok], block[:, tok:])
        acc = None
        for k in range(4):
            fetch(k).wait()
            part = dot(wbuf[k], obuf[k], ((1,), (0,)))
            acc = part if acc is None else acc + part
        pre = pre_ref[...]
        cube = GELU_B * pre * pre
        t = jnp.tanh(GELU_A * (pre + cube * pre))
        slope = 0.5 * (1.0 + t) + 0.5 * pre * (1.0 - t * t) * (GELU_A * (1.0 + 3.0 * cube))
        gp = (acc * slope * (inv_ref[0:1, :] * live_row(sc, tok))).astype(BF16)
        gp_ref[...] = gp
        rd = jnp.sum(gp.astype(F32) * pre, axis=0, keepdims=True)
        rd_ref[...] = jnp.broadcast_to(rd, rd_ref.shape)

    return call(
        body,
        [
            ((ff, cols), BF16),
            ((8, cols), F32),
            ((4, quarter, cols), BF16),
        ]
        + [((4, quarter, tok), BF16)] * 3,
        [(sc, S), (down, H)] + [(a, V) for a in (*own, *other)] + [(pre, V), (inv, V)],
        [
            pltpu.VMEM((4, ff, pair), BF16),
            pltpu.VMEM((4, pair, cols), BF16),
            pltpu.SemaphoreType.DMA((4,)),
        ],
        flops=2 * d * ff * cols,
        moved_bytes=d * ff * 2,
        limit=20,
    )


def normed_part(sc, up, gp, rd):
    d, ff = up.shape
    pair = d // 4
    width = pair // 2
    cols = gp.shape[1]

    def body(sc, up_ref, gp_ref, rd_ref, pown_ref, psib_ref, wbuf, sem):
        y, c = sc[1], sc[3]

        def fetch(k):
            start = pl.multiple_of(((y + k) % 4) * pair, pair)
            return pltpu.make_async_copy(up_ref.at[pl.ds(start, pair), :], wbuf.at[k], sem.at[k])

        for k in range(4):
            fetch(k).start()
        mine = pl.multiple_of(c * width, width)
        its = pl.multiple_of((1 - c) * width, width)
        gp = gp_ref[...]
        for k in range(4):
            fetch(k).wait()
            psib_ref[k, :width, :] = dot(wbuf[k, pl.ds(its, width), :], gp, ((1,), (0,))).astype(BF16)
            pown_ref[k] = dot(wbuf[k, pl.ds(mine, width), :], gp, ((1,), (0,)))
            psib_ref[k, width:, :] = extra_rows(rd_ref[0:1, :])

    return call(
        body,
        [((4, width, cols), F32), ((4, width + EXTRA, cols), BF16)],
        [(sc, S), (up, H), (gp, V), (rd, V)],
        [pltpu.VMEM((4, pair, ff), BF16), pltpu.SemaphoreType.DMA((4,))],
        flops=2 * d * ff * cols,
        moved_bytes=d * ff * 2,
        limit=20,
    )


def pair_sum(pown, psib, rd):
    width, cols = pown.shape[1:]

    def body(p_ref, s_ref, rd_ref, q0, rd0, q1, q2, q3):
        total = rd_ref[0:1, :] + sum_extra(s_ref[0, width:, :])
        q0[...] = p_ref[0] + s_ref[0, :width, :].astype(F32)
        rd0[...] = jnp.broadcast_to(total, rd0.shape)
        tail = extra_rows(total)
        for k, ref in ((1, q1), (2, q2), (3, q3)):
            ref[:width, :] = (p_ref[k] + s_ref[k, :width, :].astype(F32)).astype(BF16)
            ref[width:, :] = tail

    return call(
        body,
        [((width, cols), F32), ((8, cols), F32)] + [((width + EXTRA, cols), BF16)] * 3,
        [(pown, V), (psib, V), (rd, V)],
    )


def input_grad(sc, q0, rd0, recv, hidden_t, out_t, gain_mat, inv, inv_count):
    micro, width, tok = hidden_t.shape

    def body(sc, q0, rd0, r1, r2, r3, h_ref, o_ref, g_ref, inv_ref, ic_ref, out_ref, gain_ref):
        d = 8 * width
        grad = q0[...]
        rd = rd0[0:1, :]
        for ref in (r1, r2, r3):
            grad = grad + ref[:width, :].astype(F32)
            rd = rd + sum_extra(ref[width:, :])
        live = live_row(sc, tok)
        ic = ic_ref[0:1, :]
        factor = inv_ref[0:1, :] * rd / d
        gain = jnp.zeros((width, tok), F32)
        for m in range(micro):
            cut = slice(m * tok, (m + 1) * tok)
            h = h_ref[m].astype(F32)
            scaled = (o_ref[m].astype(F32) * (live[:, cut] * ic)).astype(BF16).astype(F32)
            rest = g_ref[...] * grad[:, cut] - h * factor[:, cut]
            out_ref[m] = (scaled + rest * ic).astype(BF16)
            gain = gain + grad[:, cut] * h
        gain_ref[...] = jnp.sum(gain, axis=1, keepdims=True) * ic[:, :1]

    return call(
        body,
        [((micro, width, tok), BF16), ((width, 1), F32)],
        [(sc, S)] + [(a, V) for a in (q0, rd0, *recv, hidden_t, out_t, gain_mat, inv, inv_count)],
    )


def up_part(sc, hown, mine, its, gps):
    pair, cols = hown.shape
    width = pair // 2
    ff = gps[0].shape[0]
    rows = pair // 4

    def body(sc, hown_ref, m1, m2, m3, i1, i2, i3, g0, g1, g2, g3, b0, b1, b2, b3, hbuf, gbuf, acc):
        z, c = sc[2], sc[3]
        lo = pl.multiple_of(c * width, width)
        hi = pl.multiple_of((1 - c) * width, width)
        hbuf[:, :cols] = hown_ref[...]
        for k, (a, b) in enumerate(((m1, i1), (m2, i2), (m3, i3)), 1):
            hbuf[pl.ds(lo, width), k * cols : (k + 1) * cols] = a[...]
            hbuf[pl.ds(hi, width), k * cols : (k + 1) * cols] = b[...]
        for k, g in enumerate((g0, g1, g2, g3)):
            gbuf[:, k * cols : (k + 1) * cols] = g[...]
        acc[...] = dot(hbuf[...], gbuf[...], ((1,), (1,)))
        for k, ref in enumerate((b0, b1, b2, b3)):
            start = pl.multiple_of(((z + k) % 4) * rows, rows)
            ref[...] = acc[pl.ds(start, rows), :].astype(ref.dtype)

    return call(
        body,
        [((rows, ff), F32)] + [((rows, ff), BF16)] * 3,
        [(sc, S)] + [(a, V) for a in (hown, *mine, *its, *gps)],
        [
            pltpu.VMEM((pair, 4 * cols), BF16),
            pltpu.VMEM((ff, 4 * cols), BF16),
            pltpu.VMEM((pair, ff), F32),
        ],
        flops=2 * pair * ff * cols * 4,
        limit=20,
    )


def down_part(sc, oown, mine, its, acts):
    _, rows, cols = oown.shape
    tok = cols // 2
    ff = acts[0].shape[0]
    pair = 4 * rows

    def body(sc, oown_ref, m1, m2, m3, i1, i2, i3, a0, a1, a2, a3, b0, b1, b2, b3, obuf, abuf, acc):
        x, y, c = sc[0], sc[1], sc[3]
        for j in range(4):
            cut = slice(j * rows, (j + 1) * rows)
            obuf[cut, :cols] = oown_ref[j]
            for k, (a, b) in enumerate(((m1, i1), (m2, i2), (m3, i3)), 1):
                left, right = a[j], b[j]
                obuf[cut, k * cols : k * cols + tok] = jnp.where(c == 0, left, right)
                obuf[cut, k * cols + tok : (k + 1) * cols] = jnp.where(c == 0, right, left)
        for k, a in enumerate((a0, a1, a2, a3)):
            abuf[:, k * cols : (k + 1) * cols] = a[...]
        acc[...] = dot(obuf[...], abuf[...], ((1,), (1,)))
        for k, ref in enumerate((b0, b1, b2, b3)):
            start = pl.multiple_of(((y - x - k + 8) % 4) * rows, rows)
            ref[...] = acc[pl.ds(start, rows), :].astype(ref.dtype)

    return call(
        body,
        [((rows, ff), F32)] + [((rows, ff), BF16)] * 3,
        [(sc, S)] + [(a, V) for a in (oown, *mine, *its, *acts)],
        [
            pltpu.VMEM((pair, 4 * cols), BF16),
            pltpu.VMEM((ff, 4 * cols), BF16),
            pltpu.VMEM((pair, ff), F32),
        ],
        flops=2 * pair * ff * cols * 4,
        limit=20,
    )


def at_owner(blocks, axis):
    return (blocks[0],) + tuple(moved(blocks[k], axis, k) for k in (1, 2, 3))


def add_up(blocks, inv_count):
    first, *rest = blocks

    def body(own, r1, r2, r3, ic_ref, out_ref):
        total = own[...] + r1[...].astype(F32) + (r2[...].astype(F32) + r3[...].astype(F32))
        out_ref[...] = total * ic_ref[0:1, 0:1]

    return call(body, [(first.shape, F32)], [(a, V) for a in (first, *rest, inv_count)])[0]


def on_device(hidden_in, out_grad, pack_fill, norm_gain, up_weight, down_weight):
    hidden_t = jnp.swapaxes(hidden_in, 1, 2)
    out_t = jnp.swapaxes(out_grad, 1, 2)
    _, width, tok = hidden_t.shape
    fills = pack_fill[:, 0]
    place = [lax.axis_index(a) for a in ("x", "y", "z", "c")]
    sc = jnp.concatenate([jnp.stack(place).astype(jnp.int32), fills, jnp.zeros((2,), jnp.int32)])
    gain_mat = jnp.broadcast_to(norm_gain[:, None], (width, tok))

    payload = prepare(hidden_t, gain_mat)
    h_own = (payload,) + ring_of(payload, "y")
    h_other = tuple(moved(a, "c", 1) for a in h_own)
    o_own = (out_t,) + ring_of(out_t, "y")
    o_other = tuple(moved(a, "c", 1) for a in o_own)

    count = jnp.broadcast_to(jnp.sum(fills).astype(F32), (8, 128))
    inv_count = 1.0 / total_over(count, ("x", "z"))

    act, pre, inv, h_home, *h_send = forward_part(sc, up_weight, h_own, h_other)
    acts = (act,) + ring_of(act, "z")
    h_mine = tuple(moved(a, "x", k) for k, a in enumerate(h_send, 1))
    h_its = tuple(moved(a, "c", 1) for a in h_mine)

    gp, rd, o_home, *o_send = backward_part(sc, down_weight, o_own, o_other, pre, inv)
    gps = (gp,) + ring_of(gp, "x")
    o_mine = tuple(moved(a, "z", k) for k, a in enumerate(o_send, 1))
    o_its = tuple(moved(a, "c", 1) for a in o_mine)

    pown, psib = normed_part(sc, up_weight, gp, rd)
    q0, rd0, *q_send = pair_sum(pown, moved(psib, "c", 1), rd)
    q_recv = tuple(moved(a, "y", k) for k, a in enumerate(q_send, 1))
    in_t, gain = input_grad(sc, q0, rd0, q_recv, hidden_t, out_t, gain_mat, inv, inv_count)
    gain_grad = total_over(gain[:, 0], ("x", "z"))

    down_blocks = at_owner(down_part(sc, o_home, o_mine, o_its, acts), "x")
    up_blocks = at_owner(up_part(sc, h_home, h_mine, h_its, gps), "z")
    down_grad = add_up(down_blocks, inv_count).T
    up_grad = add_up(up_blocks, inv_count)
    return (jnp.swapaxes(in_t, 1, 2), up_grad, down_grad, gain_grad)


def solution(mesh):
    split = Mesh(mesh.devices.reshape(4, 4, 4, 2), ("x", "z", "y", "c"))
    dp, mp = ("x", "z"), ("y", "c")
    in_specs = (
        P(None, dp, mp),
        P(None, dp, mp),
        P(None, dp),
        P(mp),
        P(None, mp),
        P(mp, None),
    )
    out_specs = (P(None, dp, mp), P(dp, mp), P(mp, dp), P(mp))

    return jax.shard_map(
        on_device, mesh=split, in_specs=in_specs, out_specs=out_specs, check_vma=False
    )
```

```python
import jax
import jax.numpy as jnp
from jax import lax
from jax.experimental import pallas as pl
from jax.experimental.pallas import tpu as pltpu
from jax.sharding import Mesh
from jax.sharding import PartitionSpec as P

INTERPRET = False
MIB = 1024 * 1024
EPS = 1e-06
EXTRA = 16
STAGE_LIMIT = 44
GELU_A = 0.7978845608028654
GELU_B = 0.044715

F32 = jnp.float32
BF16 = jnp.bfloat16


def moved(value, axis, step):
    size = lax.axis_size(axis)
    return lax.ppermute(value, axis, [(i, (i + step) % size) for i in range(size)])


def led(value, axis, sign):
    size = lax.axis_size(axis)
    pairs = [
        (2 * i + c, 2 * ((i + sign * (1 - 2 * c)) % size) + c) for i in range(size) for c in (0, 1)
    ]
    return lax.ppermute(value, (axis, "c"), pairs)


def gathered(value, axis):
    behind = led(value, axis, 1)
    ahead = led(value, axis, -1)
    return behind, ahead, led(behind, axis, 1)


def sibling(value):
    return moved(value, "c", 1)


def total_over(value, axes):
    for axis in axes:
        a, b, c = (moved(value, axis, step) for step in (1, 2, 3))
        value = (value + b) + (a + c)
    return value


def spec(space=pltpu.VMEM):
    return pl.BlockSpec(memory_space=space)


def call(body, outs, ins, scratch=(), flops=0, moved_bytes=0, limit=8):
    return pl.pallas_call(
        body,
        out_shape=[jax.ShapeDtypeStruct(s, d) for s, d in outs],
        in_specs=[spec(space) for _, space in ins],
        out_specs=[spec() for _ in outs],
        scratch_shapes=list(scratch),
        cost_estimate=pl.CostEstimate(flops=flops, bytes_accessed=moved_bytes, transcendentals=0),
        compiler_params=pltpu.CompilerParams(vmem_limit_bytes=limit * MIB),
        interpret=INTERPRET,
    )(*[a for a, _ in ins])


V, S, H = pltpu.VMEM, pltpu.SMEM, pltpu.HBM


def split3(value):
    hi = value.astype(BF16)
    rest = value - hi.astype(F32)
    mid = rest.astype(BF16)
    return hi, mid, (rest - mid.astype(F32)).astype(BF16)


def extra_rows(value):
    parts = [p.astype(F32) for p in split3(value)]
    row = lax.broadcasted_iota(jnp.int32, (EXTRA, value.shape[-1]), 0)
    out = jnp.where(row == 0, parts[0], 0.0)
    out = jnp.where(row == 1, parts[1], out)
    return jnp.where(row == 2, parts[2], out).astype(BF16)


def sum_extra(rows):
    return jnp.sum(rows.astype(F32), axis=0, keepdims=True)


def dot(left, right, dims):
    return lax.dot_general(left, right, (dims, ((), ())), preferred_element_type=F32)


def live_row(sc, tok):
    pos = lax.broadcasted_iota(jnp.int32, (1, 2 * tok), 1)
    in_first = pos < tok
    limit = jnp.where(in_first, sc[4], sc[5] + tok)
    return (pos < limit).astype(F32)


def gain_columns(g_ref, tok):
    return jnp.broadcast_to(g_ref[...], (tok, g_ref.shape[1])).T


OTHER = (0, 2, 1, 3)


def listed(target, here, c):
    delta = (target - here + 8) % 4
    return jnp.where(delta == 0, 0, jnp.where(delta == 2, 3, jnp.where((delta == 3) == (c == 0), 1, 2)))


def prepare(fill, hidden_t, out_t, gain):
    micro, width, tok = hidden_t.shape
    body_rows = width + EXTRA

    def body(fill_ref, h_ref, o_ref, g_ref, out_ref, count_ref):
        g = gain_columns(g_ref, tok)
        for m in range(micro):
            h = h_ref[m].astype(F32)
            out_ref[m, :width, :] = (h * g).astype(BF16)
            out_ref[m, width:body_rows, :] = extra_rows(jnp.sum(h * h, axis=0, keepdims=True))
            out_ref[m, body_rows:, :] = o_ref[m]
        count_ref[...] = jnp.full(count_ref.shape, (fill_ref[0, 0] + fill_ref[1, 0]).astype(F32))

    return call(
        body,
        [((micro, body_rows + width, tok), BF16), ((8, 128), F32)],
        [(fill, S), (hidden_t, V), (out_t, V), (gain, V)],
    )


def stage_weights(sc, up, down):
    d, ff = up.shape
    pair = d // 4

    def body(sc, up_ref, down_ref, upv, downv, sem):
        y, c = sc[1], sc[3]
        s = 1 - 2 * c
        copies = []
        for k, chip in enumerate((y, y - s, y + s, y + 2)):
            start = pl.multiple_of(((chip + 4) % 4) * pair, pair)
            copies.append(
                pltpu.make_async_copy(up_ref.at[pl.ds(start, pair), :], upv.at[k], sem.at[k])
            )
            copies.append(
                pltpu.make_async_copy(down_ref.at[:, pl.ds(start, pair)], downv.at[k], sem.at[4 + k])
            )
        for copy in copies:
            copy.start()
        for copy in copies:
            copy.wait()

    return call(
        body,
        [((4, pair, ff), BF16), ((4, ff, pair), BF16)],
        [(sc, S), (up, H), (down, H)],
        [pltpu.SemaphoreType.DMA((8,))],
        flops=10**9,
        moved_bytes=4 * d * ff,
        limit=STAGE_LIMIT,
    )


def mlp(sc, upv, downv, own, other):
    micro, padded, tok = own[0].shape
    width = (padded - EXTRA) // 2
    below = width + EXTRA
    pair = 2 * width
    quarter = pair // 4
    ff = upv.shape[2]
    d = 4 * pair
    cols = micro * tok

    def body(sc, up_ref, down_ref, *refs):
        r, t = refs[0:4], refs[4:8]
        act_ref, gp_ref, inv_ref, rd_ref, hown, ha, h2, oown, oa, o2, hbuf, obuf = refs[8:]
        x, y, z, c = sc[0], sc[1], sc[2], sc[3]
        s = 1 - 2 * c
        mine = pl.multiple_of(c * width, width)
        its = pl.multiple_of((1 - c) * width, width)
        squares = []
        for m in range(micro):
            cut = slice(m * tok, (m + 1) * tok)
            total = jnp.zeros((1, tok), F32)
            for k in range(4):
                a, b = r[k], t[OTHER[k]]
                hbuf[k, pl.ds(mine, width), cut] = a[m, :width, :]
                hbuf[k, pl.ds(its, width), cut] = b[m, :width, :]
                obuf[k, pl.ds(mine, width), cut] = a[m, below:, :]
                obuf[k, pl.ds(its, width), cut] = b[m, below:, :]
                total = total + sum_extra(a[m, width:below, :]) + sum_extra(b[m, width:below, :])
            squares.append(total)
        inv = lax.rsqrt(jnp.concatenate(squares, axis=1) / d + EPS)
        inv_ref[...] = jnp.broadcast_to(inv, inv_ref.shape)
        hown[...] = hbuf[listed(x, y, c)]
        ha[...] = hbuf[listed(x + s, y, c)]
        h2[...] = hbuf[listed(x + 2, y, c), pl.ds(mine, width), :]
        for ref, place in ((oown, z), (oa, z + s), (o2, z + 2)):
            row = pl.multiple_of(((place + 4) % 4) * quarter, quarter)
            for j in range(4):
                block = obuf[j, pl.ds(row, quarter), :]
                if ref is o2:
                    block = jnp.where(c == 0, block[:, :tok], block[:, tok:])
                ref[j] = block
        acc = dot(hbuf[0].T, up_ref[0], ((1,), (0,)))
        for k in range(1, 4):
            acc = acc + dot(hbuf[k].T, up_ref[k], ((1,), (0,)))
        pre = acc.T * inv
        live = live_row(sc, tok)
        cube = GELU_B * pre * pre
        th = jnp.tanh(GELU_A * (pre + cube * pre))
        act_ref[...] = (0.5 * pre * (1.0 + th) * live).astype(BF16)
        slope = 0.5 * (1.0 + th) + 0.5 * pre * (1.0 - th * th) * (GELU_A * (1.0 + 3.0 * cube))
        acc = dot(down_ref[0], obuf[0], ((1,), (0,)))
        for k in range(1, 4):
            acc = acc + dot(down_ref[k], obuf[k], ((1,), (0,)))
        gp = (acc * slope * (inv * live)).astype(BF16)
        gp_ref[...] = gp
        rd = jnp.sum(gp.astype(F32) * pre, axis=0, keepdims=True)
        rd_ref[...] = jnp.broadcast_to(rd, rd_ref.shape)

    return call(
        body,
        [
            ((ff, cols), BF16),
            ((ff, cols), BF16),
            ((8, cols), F32),
            ((8, cols), F32),
            ((pair, cols), BF16),
            ((pair, cols), BF16),
            ((width, cols), BF16),
            ((4, quarter, cols), BF16),
            ((4, quarter, cols), BF16),
            ((4, quarter, tok), BF16),
        ],
        [(sc, S), (upv, V), (downv, V)] + [(a, V) for a in (*own, *other)],
        [pltpu.VMEM((4, pair, cols), BF16), pltpu.VMEM((4, pair, cols), BF16)],
        flops=4 * d * ff * cols,
        moved_bytes=d * ff * 4,
        limit=16,
    )


def normed_part(sc, upv, gp, rd):
    _, pair, ff = upv.shape
    width = pair // 2
    cols = gp.shape[1]

    def body(sc, up_ref, gp_ref, rd_ref, pown_ref, psib_ref):
        c = sc[3]
        mine = pl.multiple_of(c * width, width)
        its = pl.multiple_of((1 - c) * width, width)
        gp = gp_ref[...]
        tail = extra_rows(rd_ref[0:1, :])
        for k in range(4):
            j = OTHER[k]
            psib_ref[j, :width, :] = dot(up_ref[k, pl.ds(its, width), :], gp, ((1,), (0,))).astype(BF16)
            psib_ref[j, width:, :] = tail
            pown_ref[k] = dot(up_ref[k, pl.ds(mine, width), :], gp, ((1,), (0,)))

    return call(
        body,
        [((4, width, cols), F32), ((4, width + EXTRA, cols), BF16)],
        [(sc, S), (upv, V), (gp, V), (rd, V)],
        flops=8 * pair * ff * cols,
        moved_bytes=8 * pair * ff,
    )


def pair_sum(pown, psib, rd):
    width, cols = pown.shape[1:]

    def body(p_ref, s_ref, rd_ref, q0, rd0, q1, q2, q3):
        total = rd_ref[0:1, :] + sum_extra(s_ref[0, width:, :])
        q0[...] = p_ref[0] + s_ref[0, :width, :].astype(F32)
        rd0[...] = jnp.broadcast_to(total, rd0.shape)
        tail = extra_rows(total)
        for k, ref in ((1, q1), (2, q2), (3, q3)):
            ref[:width, :] = (p_ref[k] + s_ref[k, :width, :].astype(F32)).astype(BF16)
            ref[width:, :] = tail

    return call(
        body,
        [((width, cols), F32), ((8, cols), F32)] + [((width + EXTRA, cols), BF16)] * 3,
        [(pown, V), (psib, V), (rd, V)],
    )


def input_grad(sc, q0, rd0, recv, hidden_t, out_t, gain, inv, inv_count):
    micro, width, tok = hidden_t.shape

    def body(sc, q0, rd0, r1, r2, r3, h_ref, o_ref, g_ref, inv_ref, ic_ref, out_ref, gain_ref):
        d = 8 * width
        grad = q0[...]
        rd = rd0[0:1, :]
        for ref in (r1, r2, r3):
            grad = grad + ref[:width, :].astype(F32)
            rd = rd + sum_extra(ref[width:, :])
        live = live_row(sc, tok)
        ic = ic_ref[0:1, :]
        g = gain_columns(g_ref, tok)
        factor = inv_ref[0:1, :] * rd / d
        total = jnp.zeros((width, tok), F32)
        for m in range(micro):
            cut = slice(m * tok, (m + 1) * tok)
            h = h_ref[m].astype(F32)
            scaled = (o_ref[m].astype(F32) * (live[:, cut] * ic)).astype(BF16).astype(F32)
            rest = g * grad[:, cut] - h * factor[:, cut]
            out_ref[m] = (scaled + rest * ic).astype(BF16)
            total = total + grad[:, cut] * h
        gain_ref[...] = jnp.sum(total, axis=1, keepdims=True) * ic[:, :1]

    return call(
        body,
        [((micro, width, tok), BF16), ((width, 1), F32)],
        [(sc, S)] + [(a, V) for a in (q0, rd0, *recv, hidden_t, out_t, gain, inv, inv_count)],
    )


def gradient_start(lefts, rights, micro_rows=False):
    rows = lefts[0].shape[0] * (lefts[0].shape[1] if micro_rows else 1)
    cols = rights[0].shape[1]
    ff = rights[0].shape[0]

    def body(l0, l1, l2, r0, r1, r2, acc_ref, lbuf, rbuf):
        for k, (left, right) in enumerate(((l0, r0), (l1, r1), (l2, r2))):
            cut = slice(k * cols, (k + 1) * cols)
            rbuf[:, cut] = right[...]
            if micro_rows:
                size = left.shape[1]
                for j in range(4):
                    lbuf[j * size : (j + 1) * size, cut] = left[OTHER[j] if k == 2 else j]
            else:
                lbuf[:, cut] = left[...]
        acc_ref[...] = dot(lbuf[...], rbuf[...], ((1,), (1,)))

    return call(
        body,
        [((rows, ff), F32)],
        [(a, V) for a in (*lefts, *rights)],
        [pltpu.VMEM((rows, 3 * cols), BF16), pltpu.VMEM((ff, 3 * cols), BF16)],
        flops=2 * rows * ff * cols * 3,
        limit=12,
    )[0]


def up_finish(sc, acc, mine, its, gp):
    width, cols = mine.shape
    ff = gp.shape[0]
    rows = width // 2

    def body(sc, acc_ref, m_ref, i_ref, g_ref, b0, b1, b2, b3, lbuf, total):
        z, c = sc[2], sc[3]
        lbuf[pl.ds(pl.multiple_of(c * width, width), width), :] = m_ref[...]
        lbuf[pl.ds(pl.multiple_of((1 - c) * width, width), width), :] = i_ref[...]
        total[...] = acc_ref[...] + dot(lbuf[...], g_ref[...], ((1,), (1,)))
        for k, ref in enumerate((b0, b1, b2, b3)):
            start = pl.multiple_of(((z + k) % 4) * rows, rows)
            ref[...] = total[pl.ds(start, rows), :].astype(ref.dtype)

    return call(
        body,
        [((rows, ff), F32)] + [((rows, ff), BF16)] * 3,
        [(sc, S)] + [(a, V) for a in (acc, mine, its, gp)],
        [pltpu.VMEM((2 * width, cols), BF16), pltpu.VMEM((2 * width, ff), F32)],
        flops=4 * width * ff * cols,
        limit=12,
    )


def down_finish(sc, acc, mine, its, act):
    _, rows, tok = mine.shape
    ff, cols = act.shape

    def body(sc, acc_ref, m_ref, i_ref, a_ref, b0, b1, b2, b3, lbuf, total):
        x, y, c = sc[0], sc[1], sc[3]
        for j in range(4):
            cut = slice(j * rows, (j + 1) * rows)
            left, right = m_ref[j], i_ref[OTHER[j]]
            lbuf[cut, :tok] = jnp.where(c == 0, left, right)
            lbuf[cut, tok:] = jnp.where(c == 0, right, left)
        total[...] = acc_ref[...] + dot(lbuf[...], a_ref[...], ((1,), (1,)))
        for k, ref in enumerate((b0, b1, b2, b3)):
            start = pl.multiple_of(listed(x + k, y, c) * rows, rows)
            ref[...] = total[pl.ds(start, rows), :].astype(ref.dtype)

    return call(
        body,
        [((rows, ff), F32)] + [((rows, ff), BF16)] * 3,
        [(sc, S)] + [(a, V) for a in (acc, mine, its, act)],
        [pltpu.VMEM((4 * rows, cols), BF16), pltpu.VMEM((4 * rows, ff), F32)],
        flops=8 * rows * ff * cols,
        limit=12,
    )


def at_owner(blocks, axis):
    return (blocks[0],) + tuple(moved(blocks[k], axis, k) for k in (1, 2, 3))


def add_up(blocks, inv_count):
    first, *rest = blocks

    def body(own, r1, r2, r3, ic_ref, out_ref):
        total = own[...] + r1[...].astype(F32) + (r2[...].astype(F32) + r3[...].astype(F32))
        out_ref[...] = total * ic_ref[0:1, 0:1]

    return call(body, [(first.shape, F32)], [(a, V) for a in (first, *rest, inv_count)])[0]


def on_device(hidden_in, out_grad, pack_fill, norm_gain, up_weight, down_weight):
    hidden_t = jnp.swapaxes(hidden_in, 1, 2)
    out_t = jnp.swapaxes(out_grad, 1, 2)
    gain_row = norm_gain[None, :]
    place = [lax.axis_index(a) for a in ("x", "y", "z", "c")]
    sc = jnp.concatenate(
        [jnp.stack(place).astype(jnp.int32), pack_fill[:, 0], jnp.zeros((2,), jnp.int32)]
    )

    payload, count = prepare(pack_fill, hidden_t, out_t, gain_row)
    own = (payload, *gathered(payload, "y"))
    other = tuple(sibling(a) for a in own)
    upv, downv = stage_weights(sc, up_weight, down_weight)
    inv_count = 1.0 / total_over(count, ("x", "z"))

    act, gp, inv, rd, h_own, h_a, h_2, o_own, o_a, o_2 = mlp(sc, upv, downv, own, other)
    gps = gathered(gp, "x")
    acts = gathered(act, "z")
    h_a = led(h_a, "x", 1)
    o_a = led(o_a, "z", 1)
    h_2 = moved(h_2, "x", 2)
    o_2 = moved(o_2, "z", 2)

    pown, psib = normed_part(sc, upv, gp, rd)
    q0, rd0, *q_send = pair_sum(pown, sibling(psib), rd)
    q_recv = (led(q_send[0], "y", -1), led(q_send[1], "y", 1), moved(q_send[2], "y", 2))

    up_acc = gradient_start((h_own, h_a, sibling(h_a)), (gp, *gps[:2]))
    down_acc = gradient_start((o_own, o_a, sibling(o_a)), (act, *acts[:2]), True)
    up_blocks = at_owner(up_finish(sc, up_acc, h_2, sibling(h_2), gps[2]), "z")
    down_blocks = at_owner(down_finish(sc, down_acc, o_2, sibling(o_2), acts[2]), "x")

    in_t, gain = input_grad(sc, q0, rd0, q_recv, hidden_t, out_t, gain_row, inv, inv_count)
    gain_grad = total_over(gain[:, 0], ("x", "z"))
    up_grad = add_up(up_blocks, inv_count)
    down_grad = add_up(down_blocks, inv_count).T
    return (jnp.swapaxes(in_t, 1, 2), up_grad, down_grad, gain_grad)


def solution(mesh):
    split = Mesh(mesh.devices.reshape(4, 4, 4, 2), ("x", "z", "y", "c"))
    dp, mp = ("x", "z"), ("y", "c")
    in_specs = (
        P(None, dp, mp),
        P(None, dp, mp),
        P(None, dp),
        P(mp),
        P(None, mp),
        P(mp, None),
    )
    out_specs = (P(None, dp, mp), P(dp, mp), P(mp, dp), P(mp))

    return jax.shard_map(
        on_device, mesh=split, in_specs=in_specs, out_specs=out_specs, check_vma=False
    )
```

```python
import jax
import jax.numpy as jnp
from jax import lax
from jax.experimental import pallas as pl
from jax.experimental.pallas import tpu as pltpu
from jax.sharding import Mesh
from jax.sharding import PartitionSpec as P

INTERPRET = False
MIB = 1024 * 1024
EPS = 1e-06
EXTRA = 16
STAGE_LIMIT = 41
GELU_A = 0.7978845608028654
GELU_B = 0.044715

F32 = jnp.float32
BF16 = jnp.bfloat16


def moved(value, axis, step):
    size = lax.axis_size(axis)
    return lax.ppermute(value, axis, [(i, (i + step) % size) for i in range(size)])


def led(value, axis, sign):
    size = lax.axis_size(axis)
    pairs = [
        (2 * i + c, 2 * ((i + sign * (1 - 2 * c)) % size) + c) for i in range(size) for c in (0, 1)
    ]
    return lax.ppermute(value, (axis, "c"), pairs)


def gathered(forward, back, axis):
    behind = led(forward, axis, 1)
    ahead = led(back, axis, -1)
    return behind, ahead, led(behind, axis, 1)


def sibling(value):
    return moved(value, "c", 1)


def total_over(value, axes):
    for axis in axes:
        a, b, c = (moved(value, axis, step) for step in (1, 2, 3))
        value = (value + b) + (a + c)
    return value


def spec(space=pltpu.VMEM):
    return pl.BlockSpec(memory_space=space)


def call(body, outs, ins, scratch=(), flops=0, moved_bytes=0, limit=8):
    return pl.pallas_call(
        body,
        out_shape=[jax.ShapeDtypeStruct(s, d) for s, d in outs],
        in_specs=[spec(space) for _, space in ins],
        out_specs=[spec() for _ in outs],
        scratch_shapes=list(scratch),
        cost_estimate=pl.CostEstimate(flops=flops, bytes_accessed=moved_bytes, transcendentals=0),
        compiler_params=pltpu.CompilerParams(vmem_limit_bytes=limit * MIB),
        interpret=INTERPRET,
    )(*[a for a, _ in ins])


V, S, H = pltpu.VMEM, pltpu.SMEM, pltpu.HBM


def split3(value):
    hi = value.astype(BF16)
    rest = value - hi.astype(F32)
    mid = rest.astype(BF16)
    return hi, mid, (rest - mid.astype(F32)).astype(BF16)


def extra_rows(value):
    parts = [p.astype(F32) for p in split3(value)]
    row = lax.broadcasted_iota(jnp.int32, (EXTRA, value.shape[-1]), 0)
    out = jnp.where(row == 0, parts[0], 0.0)
    out = jnp.where(row == 1, parts[1], out)
    return jnp.where(row == 2, parts[2], out).astype(BF16)


def sum_extra(rows):
    return jnp.sum(rows.astype(F32), axis=0, keepdims=True)


def dot(left, right, dims):
    return lax.dot_general(left, right, (dims, ((), ())), preferred_element_type=F32)


def live_row(sc, tok):
    pos = lax.broadcasted_iota(jnp.int32, (1, 2 * tok), 1)
    in_first = pos < tok
    limit = jnp.where(in_first, sc[4], sc[5] + tok)
    return (pos < limit).astype(F32)


def gain_columns(g_ref, tok):
    return jnp.broadcast_to(g_ref[...], (tok, g_ref.shape[1])).T


OTHER = (0, 2, 1, 3)


def listed(target, here, c):
    delta = (target - here + 8) % 4
    return jnp.where(delta == 0, 0, jnp.where(delta == 2, 3, jnp.where((delta == 3) == (c == 0), 1, 2)))


def prepare(hidden_t, out_t, gain):
    micro, width, tok = hidden_t.shape
    body_rows = width + EXTRA

    def body(h_ref, o_ref, g_ref, out_ref):
        g = gain_columns(g_ref, tok)
        for m in range(micro):
            h = h_ref[m].astype(F32)
            out_ref[m, :width, :] = (h * g).astype(BF16)
            out_ref[m, width:body_rows, :] = extra_rows(jnp.sum(h * h, axis=0, keepdims=True))
            out_ref[m, body_rows:, :] = o_ref[m]

    return call(
        body, [((micro, body_rows + width, tok), BF16)], [(hidden_t, V), (out_t, V), (gain, V)]
    )[0]


def own_count(sc):
    def body(sc, count_ref):
        count_ref[...] = jnp.full(count_ref.shape, (sc[4] + sc[5]).astype(F32))

    return call(body, [((8, 128), F32)], [(sc, S)])[0]


def stage_weights(sc, up, down):
    d, ff = up.shape
    pair = d // 4

    def body(sc, up_ref, down_ref, upv, downv, sem):
        y, c = sc[1], sc[3]
        s = 1 - 2 * c
        copies = []
        for k, chip in enumerate((y, y - s, y + s, y + 2)):
            start = pl.multiple_of(((chip + 4) % 4) * pair, pair)
            copies.append(
                pltpu.make_async_copy(up_ref.at[pl.ds(start, pair), :], upv.at[k], sem.at[k])
            )
            copies.append(
                pltpu.make_async_copy(down_ref.at[:, pl.ds(start, pair)], downv.at[k], sem.at[4 + k])
            )
        for copy in copies:
            copy.start()
        for copy in copies:
            copy.wait()

    return call(
        body,
        [((4, pair, ff), BF16), ((4, ff, pair), BF16)],
        [(sc, S), (up, H), (down, H)],
        [pltpu.SemaphoreType.DMA((8,))],
        flops=10**9,
        moved_bytes=4 * d * ff,
        limit=STAGE_LIMIT,
    )


def mlp(sc, upv, downv, own, other):
    micro, padded, tok = own[0].shape
    width = (padded - EXTRA) // 2
    below = width + EXTRA
    pair = 2 * width
    quarter = pair // 4
    ff = upv.shape[2]
    d = 4 * pair
    cols = micro * tok

    def body(sc, up_ref, down_ref, *refs):
        r, t = refs[0:4], refs[4:8]
        a1, a2, g1, g2, inv_ref, rd_ref, hown, ha, oown, oa, hbuf, obuf = refs[8:]
        x, y, z, c = sc[0], sc[1], sc[2], sc[3]
        s = 1 - 2 * c
        mine = pl.multiple_of(c * width, width)
        its = pl.multiple_of((1 - c) * width, width)
        squares = []
        for m in range(micro):
            cut = slice(m * tok, (m + 1) * tok)
            total = jnp.zeros((1, tok), F32)
            for k in range(4):
                a, b = r[k], t[OTHER[k]]
                hbuf[k, pl.ds(mine, width), cut] = a[m, :width, :]
                hbuf[k, pl.ds(its, width), cut] = b[m, :width, :]
                obuf[k, pl.ds(mine, width), cut] = a[m, below:, :]
                obuf[k, pl.ds(its, width), cut] = b[m, below:, :]
                total = total + sum_extra(a[m, width:below, :]) + sum_extra(b[m, width:below, :])
            squares.append(total)
        inv = lax.rsqrt(jnp.concatenate(squares, axis=1) / d + EPS)
        inv_ref[...] = jnp.broadcast_to(inv, inv_ref.shape)
        hown[...] = hbuf[listed(x, y, c)]
        ha[...] = hbuf[listed(x + s, y, c)]
        g1[ff:, :] = hbuf[listed(x + 2, y, c), pl.ds(mine, width), :]
        for ref, place in ((oown, z), (oa, z + s)):
            row = pl.multiple_of(((place + 4) % 4) * quarter, quarter)
            for j in range(4):
                ref[j] = obuf[j, pl.ds(row, quarter), :]
        row = pl.multiple_of(((z + 2) % 4) * quarter, quarter)
        for i, (j0, j1) in enumerate(((0, 1), (3, 2))):
            a1[ff + i * quarter : ff + (i + 1) * quarter, :] = obuf[
                jnp.where(c == 0, j0, j1), pl.ds(row, quarter), :
            ]
        acc = dot(hbuf[0].T, up_ref[0], ((1,), (0,)))
        for k in range(1, 4):
            acc = acc + dot(hbuf[k].T, up_ref[k], ((1,), (0,)))
        pre = acc.T * inv
        live = live_row(sc, tok)
        cube = GELU_B * pre * pre
        th = jnp.tanh(GELU_A * (pre + cube * pre))
        act = (0.5 * pre * (1.0 + th) * live).astype(BF16)
        a1[:ff, :] = act
        a2[...] = act
        slope = 0.5 * (1.0 + th) + 0.5 * pre * (1.0 - th * th) * (GELU_A * (1.0 + 3.0 * cube))
        acc = dot(down_ref[0], obuf[0], ((1,), (0,)))
        for k in range(1, 4):
            acc = acc + dot(down_ref[k], obuf[k], ((1,), (0,)))
        gp = (acc * slope * (inv * live)).astype(BF16)
        g1[:ff, :] = gp
        g2[...] = gp
        rd = jnp.sum(gp.astype(F32) * pre, axis=0, keepdims=True)
        rd_ref[...] = jnp.broadcast_to(rd, rd_ref.shape)

    return call(
        body,
        [
            ((ff + width, cols), BF16),
            ((ff, cols), BF16),
            ((ff + width, cols), BF16),
            ((ff, cols), BF16),
            ((8, cols), F32),
            ((8, cols), F32),
            ((pair, cols), BF16),
            ((pair, cols), BF16),
            ((4, quarter, cols), BF16),
            ((4, quarter, cols), BF16),
        ],
        [(sc, S), (upv, V), (downv, V)] + [(a, V) for a in (*own, *other)],
        [pltpu.VMEM((4, pair, cols), BF16), pltpu.VMEM((4, pair, cols), BF16)],
        flops=4 * d * ff * cols,
        moved_bytes=d * ff * 4,
        limit=16,
    )


def normed_part(sc, upv, gp, rd):
    _, pair, ff = upv.shape
    width = pair // 2
    cols = gp.shape[1]

    def body(sc, up_ref, gp_ref, rd_ref, pown_ref, psib_ref):
        c = sc[3]
        mine = pl.multiple_of(c * width, width)
        its = pl.multiple_of((1 - c) * width, width)
        gp = gp_ref[...]
        tail = extra_rows(rd_ref[0:1, :])
        for k in range(4):
            j = OTHER[k]
            psib_ref[j, :width, :] = dot(up_ref[k, pl.ds(its, width), :], gp, ((1,), (0,))).astype(BF16)
            psib_ref[j, width:, :] = tail
            pown_ref[k] = dot(up_ref[k, pl.ds(mine, width), :], gp, ((1,), (0,)))

    return call(
        body,
        [((4, width, cols), F32), ((4, width + EXTRA, cols), BF16)],
        [(sc, S), (upv, V), (gp, V), (rd, V)],
        flops=8 * pair * ff * cols,
        moved_bytes=8 * pair * ff,
    )


def pair_sum(pown, psib, rd):
    width, cols = pown.shape[1:]

    def body(p_ref, s_ref, rd_ref, q0, rd0, q1, q2, q3):
        total = rd_ref[0:1, :] + sum_extra(s_ref[0, width:, :])
        q0[...] = p_ref[0] + s_ref[0, :width, :].astype(F32)
        rd0[...] = jnp.broadcast_to(total, rd0.shape)
        tail = extra_rows(total)
        for k, ref in ((1, q1), (2, q2), (3, q3)):
            ref[:width, :] = (p_ref[k] + s_ref[k, :width, :].astype(F32)).astype(BF16)
            ref[width:, :] = tail

    return call(
        body,
        [((width, cols), F32), ((8, cols), F32)] + [((width + EXTRA, cols), BF16)] * 3,
        [(pown, V), (psib, V), (rd, V)],
    )


def input_grad(sc, q0, rd0, recv, hidden_t, out_t, gain, inv, inv_count):
    micro, width, tok = hidden_t.shape

    def body(sc, q0, rd0, r1, r2, r3, h_ref, o_ref, g_ref, inv_ref, ic_ref, out_ref, gain_ref):
        d = 8 * width
        grad = q0[...]
        rd = rd0[0:1, :]
        for ref in (r1, r2, r3):
            grad = grad + ref[:width, :].astype(F32)
            rd = rd + sum_extra(ref[width:, :])
        live = live_row(sc, tok)
        ic = ic_ref[0:1, :]
        g = gain_columns(g_ref, tok)
        factor = inv_ref[0:1, :] * rd / d
        total = jnp.zeros((width, tok), F32)
        for m in range(micro):
            cut = slice(m * tok, (m + 1) * tok)
            h = h_ref[m].astype(F32)
            scaled = (o_ref[m].astype(F32) * (live[:, cut] * ic)).astype(BF16).astype(F32)
            rest = g * grad[:, cut] - h * factor[:, cut]
            out_ref[m] = (scaled + rest * ic).astype(BF16)
            total = total + grad[:, cut] * h
        row = jnp.sum(total.T, axis=0, keepdims=True) * ic[:, :1]
        gain_ref[...] = jnp.broadcast_to(row, gain_ref.shape)

    return call(
        body,
        [((micro, width, tok), BF16), ((8, width), F32)],
        [(sc, S)] + [(a, V) for a in (q0, rd0, *recv, hidden_t, out_t, gain, inv, inv_count)],
    )


def gradient_start(lefts, rights, micro_rows=False):
    rows = lefts[0].shape[0] * (lefts[0].shape[1] if micro_rows else 1)
    ff, cols = rights[0].shape

    def body(l0, l1, l2, r0, r1, r2, acc_ref, lbuf, rbuf):
        for k, (left, right) in enumerate(((l0, r0), (l1, r1), (l2, r2))):
            cut = slice(k * cols, (k + 1) * cols)
            rbuf[:, cut] = right[:ff, :]
            if micro_rows:
                size = left.shape[1]
                for j in range(4):
                    lbuf[j * size : (j + 1) * size, cut] = left[OTHER[j] if k == 2 else j]
            else:
                lbuf[:, cut] = left[...]
        acc_ref[...] = dot(lbuf[...], rbuf[...], ((1,), (1,)))

    return call(
        body,
        [((rows, ff), F32)],
        [(a, V) for a in (*lefts, *rights)],
        [pltpu.VMEM((rows, 3 * cols), BF16), pltpu.VMEM((ff, 3 * cols), BF16)],
        flops=2 * rows * ff * cols * 3,
        limit=12,
    )[0]


def up_finish(sc, acc, mine, its, gain):
    _, cols = mine.shape
    pair, ff = acc.shape
    width = pair // 2
    rows = width // 2

    def body(sc, acc_ref, m_ref, i_ref, gain_ref, b0, b1, b2, b3, lbuf, total):
        z, c = sc[2], sc[3]
        lbuf[pl.ds(pl.multiple_of(c * width, width), width), :] = m_ref[ff:, :]
        lbuf[pl.ds(pl.multiple_of((1 - c) * width, width), width), :] = i_ref[ff:, :]
        total[...] = acc_ref[...] + dot(lbuf[...], m_ref[:ff, :], ((1,), (1,)))
        tail = extra_rows(gain_ref[0:1, :])
        for k, ref in enumerate((b0, b1, b2, b3)):
            start = pl.multiple_of(((z + k) % 4) * rows, rows)
            ref[:rows, :] = total[pl.ds(start, rows), :].astype(ref.dtype)
            if k:
                ref[rows:, :] = jnp.zeros((EXTRA, ff), BF16)
                ref[rows:, :width] = tail

    return call(
        body,
        [((rows, ff), F32)] + [((rows + EXTRA, ff), BF16)] * 3,
        [(sc, S)] + [(a, V) for a in (acc, mine, its, gain)],
        [pltpu.VMEM((pair, cols), BF16), pltpu.VMEM((pair, ff), F32)],
        flops=2 * pair * ff * cols,
        limit=12,
    )


def down_finish(sc, acc, mine, its):
    _, cols = mine.shape
    pair, ff = acc.shape
    rows = pair // 4

    def body(sc, acc_ref, m_ref, i_ref, b0, b1, b2, b3, lbuf, total):
        x, y, c = sc[0], sc[1], sc[3]
        m0, m1 = m_ref[ff : ff + rows, :], m_ref[ff + rows :, :]
        i0, i1 = i_ref[ff : ff + rows, :], i_ref[ff + rows :, :]
        for j, (first, second) in enumerate(((m0, i0), (i1, m0), (i0, m1), (m1, i1))):
            lbuf[j * rows : (j + 1) * rows, :] = jnp.where(c == 0, first, second)
        total[...] = acc_ref[...] + dot(lbuf[...], m_ref[:ff, :], ((1,), (1,)))
        for k, ref in enumerate((b0, b1, b2, b3)):
            start = pl.multiple_of(listed(x + k, y, c) * rows, rows)
            ref[...] = total[pl.ds(start, rows), :].astype(ref.dtype)

    return call(
        body,
        [((rows, ff), F32)] + [((rows, ff), BF16)] * 3,
        [(sc, S)] + [(a, V) for a in (acc, mine, its)],
        [pltpu.VMEM((pair, cols), BF16), pltpu.VMEM((pair, ff), F32)],
        flops=2 * pair * ff * cols,
        limit=12,
    )


def at_owner(blocks, axis):
    return (blocks[0],) + tuple(moved(blocks[k], axis, k) for k in (1, 2, 3))


def add_up(blocks, inv_count):
    first, *rest = blocks
    rows = first.shape[0]

    def body(own, r1, r2, r3, ic_ref, out_ref):
        parts = [r[:rows, :].astype(F32) for r in (r1, r2, r3)]
        out_ref[...] = (own[...] + parts[0] + (parts[1] + parts[2])) * ic_ref[0:1, 0:1]

    return call(body, [(first.shape, F32)], [(a, V) for a in (first, *rest, inv_count)])[0]


def gain_over_z(gain, blocks):
    width = gain.shape[1]

    def body(g_ref, r1, r2, r3, out_ref):
        total = g_ref[0:1, :]
        for r in (r1, r2, r3):
            total = total + sum_extra(r[-EXTRA:, :width])
        out_ref[...] = jnp.broadcast_to(total, out_ref.shape)

    return call(body, [(gain.shape, F32)], [(a, V) for a in (gain, *blocks)])[0]


def on_device(hidden_in, out_grad, pack_fill, norm_gain, up_weight, down_weight):
    hidden_t = jnp.swapaxes(hidden_in, 1, 2)
    out_t = jnp.swapaxes(out_grad, 1, 2)
    gain_row = norm_gain[None, :]
    place = [lax.axis_index(a) for a in ("x", "y", "z", "c")]
    sc = jnp.concatenate(
        [jnp.stack(place).astype(jnp.int32), pack_fill[:, 0], jnp.zeros((2,), jnp.int32)]
    )

    payload = prepare(hidden_t, out_t, gain_row)
    own = (payload, *gathered(payload, payload, "y"))
    other = tuple(sibling(a) for a in own)
    upv, downv = stage_weights(sc, up_weight, down_weight)
    inv_count = 1.0 / total_over(own_count(sc), ("x", "z"))

    act_all, act, gp_all, gp, inv, rd, h_own, h_a, o_own, o_a = mlp(sc, upv, downv, own, other)
    gps = gathered(gp_all, gp, "x")
    acts = gathered(act_all, act, "z")
    h_a = led(h_a, "x", 1)
    o_a = led(o_a, "z", 1)

    pown, psib = normed_part(sc, upv, gp, rd)
    q0, rd0, *q_send = pair_sum(pown, sibling(psib), rd)
    q_recv = (led(q_send[0], "y", -1), led(q_send[1], "y", 1), moved(q_send[2], "y", 2))
    in_t, gain = input_grad(sc, q0, rd0, q_recv, hidden_t, out_t, gain_row, inv, inv_count)

    up_acc = gradient_start((h_own, h_a, sibling(h_a)), (gp, *gps[:2]))
    down_acc = gradient_start((o_own, o_a, sibling(o_a)), (act, *acts[:2]), True)
    up_blocks = up_finish(sc, up_acc, gps[2], sibling(gps[2]), gain)
    up_blocks = at_owner(up_blocks, "z")
    down_blocks = down_finish(sc, down_acc, acts[2], sibling(acts[2]))
    down_blocks = at_owner(down_blocks, "x")

    gain_grad = total_over(gain_over_z(gain, up_blocks[1:]), ("x",))[0]
    up_grad = add_up(up_blocks, inv_count)
    down_grad = add_up(down_blocks, inv_count).T
    return (jnp.swapaxes(in_t, 1, 2), up_grad, down_grad, gain_grad)


def solution(mesh):
    split = Mesh(mesh.devices.reshape(4, 4, 4, 2), ("x", "z", "y", "c"))
    dp, mp = ("x", "z"), ("y", "c")
    in_specs = (
        P(None, dp, mp),
        P(None, dp, mp),
        P(None, dp),
        P(mp),
        P(None, mp),
        P(mp, None),
    )
    out_specs = (P(None, dp, mp), P(dp, mp), P(mp, dp), P(mp))

    return jax.shard_map(
        on_device, mesh=split, in_specs=in_specs, out_specs=out_specs, check_vma=False
    )
```
